768 devices in a mesh: section: 8 (over y), fsdp: 96 (over z, x, core).
Axes of the slice: x: 4, y: 8, z: 12, core: 2. Of those that a mesh axis runs over, the one named last changes fastest.
Arguments:
- master: float32 [8, 768, 4096], P('section', 'fsdp'), may hold values from -0.12 to 0.12
- first_moment: float32 [8, 768, 4096], P('section', 'fsdp'), may hold values from -0.2 to 0.2
- second_moment: float32 [8, 768, 4096], P('section', 'fsdp'), may hold values from 0.25 to 1
- gradient: float32 [8, 768, 4096], P('section', 'fsdp'), may hold values from -64 to 64
Outputs:
- new_master: float32 [8, 768, 4096], P('section', 'fsdp')
- new_first: float32 [8, 768, 4096], P('section', 'fsdp')
- new_second: float32 [8, 768, 4096], P('section', 'fsdp')
- weights: bfloat16 [8, 768, 4096], P('section')
- grad_rms: float32 [], replicated
The draws below stay inside these ranges and needn't reach their ends.
All inputs are finite; a program needn't handle non-finite values.
Results may differ from the reference program's by a relative error of at most 0.001.
Values may be sent and summed in bfloat16 or wider, within the bound.
No kernel may reach another device: no remote copies, remote signals or barrier semaphores. Data moves between devices by JAX's collectives and lax.ppermute only.
A program may use at most 64 MiB of HBM per device.

```python
import math
import jax
import jax.numpy as jnp

D = 4096
ROWS_DEV = 8
ROWS = 768
SECTIONS = 8


def draw_gradient(key, part):
    key_base = jax.random.fold_in(key, 11)
    key_rows = jax.random.fold_in(key, 12)
    key_blocks = jax.random.fold_in(key, 13)
    base = jnp.clip(jax.random.normal(key_base, (SECTIONS, ROWS, D), jnp.float32), -6.0, 6.0)
    row_scale = jnp.exp(jax.random.uniform(key_rows, (SECTIONS, ROWS, 1), jnp.float32, jnp.log(0.5), jnp.log(2.0)))
    common = jnp.zeros((1, 1, D), jnp.float32)
    block_scale = jnp.exp(jax.random.uniform(key_blocks, (SECTIONS, ROWS // ROWS_DEV, 1, 1), jnp.float32, jnp.log(0.5), jnp.log(2.0)))
    block_scale = jnp.broadcast_to(block_scale, (SECTIONS, ROWS // ROWS_DEV, ROWS_DEV, 1)).reshape(SECTIONS, ROWS, 1)
    return base * row_scale * block_scale + common


def shard_levels(own_key, shape, split, smallest, largest):
    def one(position, parts):
        heights = jax.random.uniform(jax.random.fold_in(jax.random.fold_in(own_key, 6), position), (parts,), jnp.float32, smallest / len(split), largest / len(split))
        return jnp.repeat(jnp.exp(heights), shape[position] // parts).reshape((-1,) + (1,) * (len(shape) - position - 1))

    gain = one(*split[0])
    for cut in split[1:]:
        gain = gain * one(*cut)
    return gain


def centred(key, shape, deviation, bound, split=(), dtype=jnp.bfloat16):
    array = jax.random.normal(key, shape, jnp.float32) * deviation
    if len(split) > 0:
        array = shard_levels(key, shape, split, -0.22, 0.18) * array
    return jnp.clip(array, min=-bound, max=bound).astype(dtype)


def setup_inputs(seed: int = 0) -> dict:
    seeds = jax.random.split(jax.random.key(seed), 5)
    return {
        "master": centred(seeds[0], (SECTIONS, ROWS, D), 0.02, 0.12, ((0, 8), (1, 96)), jnp.float32),
        "first_moment": centred(seeds[1], (SECTIONS, ROWS, D), 0.05, 0.2, ((0, 8), (1, 96)), jnp.float32),
        "second_moment": jnp.clip(jnp.exp(math.log(1.0) - 1.3862944 * jax.random.uniform(seeds[2], (SECTIONS, ROWS, D), jnp.float32) ** shard_levels(seeds[2], (SECTIONS, ROWS, D), ((0, 8), (1, 96)), -0.2, 0.2)), 0.25, 1.0),
        "gradient": draw_gradient(jax.random.fold_in(seeds[4], 71), 0),
    }


BETA_ONE = 0.9
BETA_TWO = 0.95
LEARN_RATE = 0.05
DECAY = 0.1
EPSILON = 1e-08
BIAS_STEPS = 10.0

def reference(master, first_moment, second_moment, gradient):
    squares = jnp.sum(gradient * gradient)
    grad_norm = jnp.sqrt(squares)
    param_count = float(SECTIONS * ROWS * D)
    limit = jnp.float32(0.5 * param_count ** 0.5)
    clip_scale = limit / jnp.maximum(grad_norm, limit)
    scaled = clip_scale * gradient
    new_first = BETA_ONE * first_moment + (1.0 - BETA_ONE) * scaled
    new_second = BETA_TWO * second_moment + (1.0 - BETA_TWO) * scaled * scaled
    first_hat = new_first / (1.0 - BETA_ONE ** BIAS_STEPS)
    second_hat = new_second / (1.0 - BETA_TWO ** BIAS_STEPS)
    update = first_hat / (jnp.sqrt(second_hat) + EPSILON)
    new_master = master * (1.0 - LEARN_RATE * DECAY) - LEARN_RATE * update
    grad_rms = grad_norm / jnp.float32(param_count ** 0.5)
    return (new_master, new_first, new_second, new_master.astype(jnp.bfloat16), grad_rms)
```

```python
import jax
import jax.numpy as jnp
from jax import lax
from jax.sharding import Mesh
from jax.sharding import PartitionSpec as P

FSDP = ("fsdp_0", "fsdp_1", "fsdp_2")


BETA_ONE = 0.9
BETA_TWO = 0.95
LEARN_RATE = 0.05
DECAY = 0.1
EPSILON = 1e-08
BIAS_STEPS = 10.0


def one_axis_at_a_time(x, axes):
    for axis in axes:
        x = lax.psum(x, axis)
    return x


def copy_for_each(x, axis):
    count = lax.axis_size(axis)
    return lax.all_to_all(jnp.broadcast_to(x[None], (count, *x.shape)), axis, 0, 0, tiled=True)


def taken_together(x, axis):
    everything = copy_for_each(x, axis)
    return jnp.sum(everything, axis=0)


def laid_out(blocks, dim):
    lengths = list(blocks.shape[1:])
    lengths[dim] *= blocks.shape[0]
    return jnp.moveaxis(blocks, 0, dim).reshape(lengths)


def all_blocks(x, axes, order):
    blocks = x[None]
    for k in order:
        blocks = lax.all_gather(blocks, axes[k], axis=0, tiled=True)
    carried = [lax.axis_size(axes[k]) for k in reversed(order)]
    blocks = blocks.reshape(*carried, *x.shape)
    turned = sorted(range(len(order)), key=lambda place: order[len(order) - 1 - place])
    return blocks.transpose(*turned, *range(len(order), blocks.ndim)).reshape(-1, *x.shape)


def gather_axes(x, axes, order, dim):
    return laid_out(all_blocks(x, axes, order), dim)


def adamw_part(master, first_moment, second_moment, gradient, clip_scale):
    scaled = clip_scale * gradient
    new_first = BETA_ONE * first_moment + (1.0 - BETA_ONE) * scaled
    new_second = BETA_TWO * second_moment + (1.0 - BETA_TWO) * scaled * scaled
    first_hat = new_first / (1.0 - BETA_ONE**BIAS_STEPS)
    second_hat = new_second / (1.0 - BETA_TWO**BIAS_STEPS)
    update = first_hat / (jnp.sqrt(second_hat) + EPSILON)
    new_master = master * (1.0 - LEARN_RATE * DECAY) - LEARN_RATE * update
    return (new_master, new_first, new_second)


def local(master, first_moment, second_moment, gradient):
    partial_sq = jnp.sum(gradient * gradient)
    squares = lax.psum(partial_sq, ("section", *FSDP))
    grad_norm = jnp.sqrt(squares)
    param_count = float(
        lax.axis_size("section")
        * lax.axis_size(FSDP)
        * gradient.shape[0]
        * gradient.shape[1]
        * gradient.shape[2]
    )
    limit = jnp.float32(0.5 * param_count**0.5)
    clip_scale = limit / jnp.maximum(grad_norm, limit)
    grad_rms = grad_norm / jnp.float32(param_count**0.5)
    new_master, new_first, new_second = adamw_part(
        master, first_moment, second_moment, gradient, clip_scale
    )
    weights = lax.all_gather(new_master.astype(jnp.bfloat16), FSDP, axis=1, tiled=True)
    return (new_master, new_first, new_second, weights, grad_rms)


def solution(mesh):
    torus = Mesh(
        mesh.devices.reshape(mesh.shape["section"], 12, 4, 2),
        ("section", "fsdp_0", "fsdp_1", "fsdp_2"),
    )
    placed = (
        P("section", FSDP, None),
        P("section", FSDP, None),
        P("section", FSDP, None),
        P("section", FSDP, None),
    )
    return jax.shard_map(
        local,
        mesh=torus,
        in_specs=placed,
        out_specs=(
            P("section", FSDP, None),
            P("section", FSDP, None),
            P("section", FSDP, None),
            P("section", None, None),
            P(),
        ),
        check_vma=False,
    )
```

```python
import jax
import jax.numpy as jnp
from jax import lax
from jax.experimental import pallas as pl
from jax.experimental.pallas import tpu as pltpu
from jax.sharding import Mesh
from jax.sharding import PartitionSpec as P

FSDP = ("fsdp_0", "fsdp_1", "fsdp_2")
NZ, NX, NC = 12, 4, 2


BETA_ONE = 0.9
BETA_TWO = 0.95
LEARN_RATE = 0.05
DECAY = 0.1
EPSILON = 1e-08
BIAS_STEPS = 10.0


def taken_together(x, axis):
    count = lax.axis_size(axis)
    everything = lax.all_to_all(jnp.broadcast_to(x, (count, 1, 1)), axis, 0, 0, tiled=True)
    return jnp.sum(everything)


def adamw_part(master, first_moment, second_moment, gradient, clip_scale):
    scaled = clip_scale * gradient
    new_first = BETA_ONE * first_moment + (1.0 - BETA_ONE) * scaled
    new_second = BETA_TWO * second_moment + (1.0 - BETA_TWO) * scaled * scaled
    first_hat = new_first / (1.0 - BETA_ONE**BIAS_STEPS)
    second_hat = new_second / (1.0 - BETA_TWO**BIAS_STEPS)
    update = first_hat / (jnp.sqrt(second_hat) + EPSILON)
    new_master = master * (1.0 - LEARN_RATE * DECAY) - LEARN_RATE * update
    return (new_master, new_first, new_second)


def pairs(target):
    found = []
    for z in range(NZ):
        for x in range(NX):
            for c in range(NC):
                tz, tx, tc = target(z, x, c)
                found.append(((z * NX + x) * NC + c, ((tz % NZ) * NX + tx % NX) * NC + tc))
    return found


def along_z(step):
    return lambda z, x, c: (z + step, x, c)


def near(step, z_core):
    def target(z, x, c):
        if c != z_core:
            return z, x + step, c
        if step == 2:
            return (z + 2 if z % 2 == 0 else z - 2), x, c
        return z + step, x, c

    return target


def from_z(k, z):
    return z + (0, -1, 1)[k] if k < 3 else z + jnp.where(z % 2 == 0, -2, 2)


def places():
    z, x, c = (lax.axis_index(a) for a in FSDP)
    rows = []
    for core in (c, 1 - c):
        for k3 in range(4):
            for k2 in range(4):
                xs = (0, -1, 1, 2)
                z0 = from_z(k3, z)
                z1 = from_z(k2, z)
                for k1 in range(3):
                    dz = (0, -4, 4)[k1]
                    first = ((z0 + dz + NZ) % NZ) * NX + (x + xs[k2] + NX) % NX
                    second = ((z1 + dz + NZ) % NZ) * NX + (x + xs[k3] + NX) % NX
                    rows.append(jnp.where(core == 0, first, second) * NC + core)
    return jnp.stack(rows).astype(jnp.int32)


def put_in_place(table, *refs):
    pieces, out, sems = refs[:8], refs[8], refs[9]
    for i, piece in enumerate(pieces):

        def start(j, _):
            pltpu.make_async_copy(piece.at[j], out.at[table[i * 12 + j]], sems.at[i * 12 + j]).start()
            return 0

        lax.fori_loop(0, 12, start, 0)
    for i, piece in enumerate(pieces):

        def finish(j, _):
            pltpu.make_async_copy(piece.at[j], out.at[table[i * 12 + j]], sems.at[i * 12 + j]).wait()
            return 0

        lax.fori_loop(0, 12, finish, 0)


def gathered(block):
    sent = lambda x, target: lax.ppermute(x, FSDP, pairs(target))
    one = jnp.concatenate([block, sent(block, along_z(4)), sent(block, along_z(-4))])
    two = jnp.concatenate([one] + [sent(one, near(s, 1)) for s in (1, -1, 2)])
    own = [two] + [sent(two, near(s, 0)) for s in (1, -1, 2)]
    other = [sent(p, lambda z, x, c: (z, x, 1 - c)) for p in own]
    out = pl.pallas_call(
        put_in_place,
        out_shape=jax.ShapeDtypeStruct((NZ * NX * NC, *block.shape[1:]), block.dtype),
        in_specs=[pl.BlockSpec(memory_space=pltpu.SMEM)] + [pl.BlockSpec(memory_space=pl.ANY)] * 8,
        out_specs=pl.BlockSpec(memory_space=pl.ANY),
        scratch_shapes=[pltpu.SemaphoreType.DMA((96,))],
        name="put_in_place",
    )(places(), *own, *other)
    return out.reshape(1, -1, block.shape[2])


def local(master, first_moment, second_moment, gradient):
    partial_sq = jnp.sum(gradient * gradient)
    squares = taken_together(taken_together(partial_sq, ("section", "fsdp_1", "fsdp_2")), "fsdp_0")
    grad_norm = jnp.sqrt(squares)
    param_count = float(
        lax.axis_size("section")
        * lax.axis_size(FSDP)
        * gradient.shape[0]
        * gradient.shape[1]
        * gradient.shape[2]
    )
    limit = jnp.float32(0.5 * param_count**0.5)
    clip_scale = limit / jnp.maximum(grad_norm, limit)
    grad_rms = grad_norm / jnp.float32(param_count**0.5)
    new_master, new_first, new_second = adamw_part(
        master, first_moment, second_moment, gradient, clip_scale
    )
    weights = gathered(new_master.astype(jnp.bfloat16))
    return (new_master, new_first, new_second, weights, grad_rms)


def solution(mesh):
    torus = Mesh(
        mesh.devices.reshape(mesh.shape["section"], NZ, NX, NC),
        ("section", *FSDP),
    )
    placed = (P("section", FSDP, None),) * 4
    return jax.shard_map(
        local,
        mesh=torus,
        in_specs=placed,
        out_specs=(
            P("section", FSDP, None),
            P("section", FSDP, None),
            P("section", FSDP, None),
            P("section", None, None),
            P(),
        ),
        check_vma=False,
    )
```

```python
import jax
import jax.numpy as jnp
from jax import lax
from jax.experimental import pallas as pl
from jax.experimental.pallas import tpu as pltpu
from jax.sharding import Mesh
from jax.sharding import PartitionSpec as P

FSDP = ("fsdp_0", "fsdp_1", "fsdp_2")
NZ, NX, NC = 12, 4, 2


BETA_ONE = 0.9
BETA_TWO = 0.95
LEARN_RATE = 0.05
DECAY = 0.1
EPSILON = 1e-08
BIAS_STEPS = 10.0


def taken_together(x, axis):
    count = lax.axis_size(axis)
    everything = lax.all_to_all(jnp.broadcast_to(x, (count, 1, 1)), axis, 0, 0, tiled=True)
    return jnp.sum(everything)


def adamw_part(master, first_moment, second_moment, gradient, clip_scale):
    scaled = clip_scale * gradient
    new_first = BETA_ONE * first_moment + (1.0 - BETA_ONE) * scaled
    new_second = BETA_TWO * second_moment + (1.0 - BETA_TWO) * scaled * scaled
    first_hat = new_first / (1.0 - BETA_ONE**BIAS_STEPS)
    second_hat = new_second / (1.0 - BETA_TWO**BIAS_STEPS)
    update = first_hat / (jnp.sqrt(second_hat) + EPSILON)
    new_master = master * (1.0 - LEARN_RATE * DECAY) - LEARN_RATE * update
    return (new_master, new_first, new_second)


def pairs(target):
    found = []
    for z in range(NZ):
        for x in range(NX):
            for c in range(NC):
                tz, tx, tc = target(z, x, c)
                found.append(((z * NX + x) * NC + c, ((tz % NZ) * NX + tx % NX) * NC + tc))
    return found


def along_z(step):
    return lambda z, x, c: (z + step, x, c)


def near(step, z_core):
    def target(z, x, c):
        if c != z_core:
            return z, x + step, c
        if step == 2:
            return (z + 2 if z % 2 == 0 else z - 2), x, c
        return z + step, x, c

    return target


def put_in_place(place, *refs):
    pieces, out, sems = refs[:8], refs[8], refs[9]
    z, x, c = place[0] // (NX * NC), place[0] // NC % NX, place[0] % NC
    by_z = (z, z + NZ - 1, z + 1, z + jnp.where(z % 2 == 0, NZ - 2, 2))
    by_x = (x, x + NX - 1, x + 1, x + 2)
    copies = []
    for i, piece in enumerate(pieces):
        core = c if i < 4 else 1 - c
        for j in range(12):
            k3, k2, k1 = i % 4, j // 3, j % 3
            row_z = jnp.where(core == 0, by_z[k3], by_z[k2]) + (0, NZ - 4, 4)[k1]
            row_x = jnp.where(core == 0, by_x[k2], by_x[k3])
            row = ((row_z % NZ) * NX + row_x % NX) * NC + core
            copies.append(pltpu.make_async_copy(piece.at[j], out.at[row], sems.at[12 * i + j]))
    for copy in copies:
        copy.start()
    for copy in copies:
        copy.wait()


def gathered(block):
    sent = lambda x, target: lax.ppermute(x, FSDP, pairs(target))
    one = jnp.concatenate([block, sent(block, along_z(4)), sent(block, along_z(-4))])
    two = jnp.concatenate([one] + [sent(one, near(s, 1)) for s in (1, -1, 2)])
    own = [two] + [sent(two, near(s, 0)) for s in (1, -1, 2)]
    other = [sent(p, lambda z, x, c: (z, x, 1 - c)) for p in own]
    out = pl.pallas_call(
        put_in_place,
        out_shape=jax.ShapeDtypeStruct((NZ * NX * NC, *block.shape[1:]), block.dtype),
        in_specs=[pl.BlockSpec(memory_space=pltpu.SMEM)] + [pl.BlockSpec(memory_space=pltpu.VMEM)] * 8,
        out_specs=pl.BlockSpec(memory_space=pl.ANY),
        scratch_shapes=[pltpu.SemaphoreType.DMA((96,))],
        name="put_in_place",
    )(lax.axis_index(FSDP).astype(jnp.int32).reshape(1), *own, *other)
    return out.reshape(1, -1, block.shape[2])


def local(master, first_moment, second_moment, gradient):
    partial_sq = jnp.sum(gradient * gradient)
    squares = taken_together(taken_together(partial_sq, ("section", "fsdp_1", "fsdp_2")), "fsdp_0")
    grad_norm = jnp.sqrt(squares)
    param_count = float(
        lax.axis_size("section")
        * lax.axis_size(FSDP)
        * gradient.shape[0]
        * gradient.shape[1]
        * gradient.shape[2]
    )
    limit = jnp.float32(0.5 * param_count**0.5)
    clip_scale = limit / jnp.maximum(grad_norm, limit)
    grad_rms = grad_norm / jnp.float32(param_count**0.5)
    new_master, new_first, new_second = adamw_part(
        master, first_moment, second_moment, gradient, clip_scale
    )
    weights = gathered(new_master.astype(jnp.bfloat16))
    return (new_master, new_first, new_second, weights, grad_rms)


def solution(mesh):
    torus = Mesh(
        mesh.devices.reshape(mesh.shape["section"], NZ, NX, NC),
        ("section", *FSDP),
    )
    placed = (P("section", FSDP, None),) * 4
    return jax.shard_map(
        local,
        mesh=torus,
        in_specs=placed,
        out_specs=(
            P("section", FSDP, None),
            P("section", FSDP, None),
            P("section", FSDP, None),
            P("section", None, None),
            P(),
        ),
        check_vma=False,
    )
```

```python
import jax
import jax.numpy as jnp
from jax import lax
from jax.experimental import pallas as pl
from jax.experimental.pallas import tpu as pltpu
from jax.sharding import Mesh
from jax.sharding import PartitionSpec as P

FSDP = ("fsdp_0", "fsdp_1", "fsdp_2")
NZ, NX, NC = 12, 4, 2


BETA_ONE = 0.9
BETA_TWO = 0.95
LEARN_RATE = 0.05
DECAY = 0.1
EPSILON = 1e-08
BIAS_STEPS = 10.0


def taken_together(x, axis):
    count = lax.axis_size(axis)
    everything = lax.all_to_all(jnp.broadcast_to(x, (count, 1, 1)), axis, 0, 0, tiled=True)
    return jnp.sum(everything)


def adamw_part(master, first_moment, second_moment, gradient, clip_scale):
    scaled = clip_scale * gradient
    new_first = BETA_ONE * first_moment + (1.0 - BETA_ONE) * scaled
    new_second = BETA_TWO * second_moment + (1.0 - BETA_TWO) * scaled * scaled
    first_hat = new_first / (1.0 - BETA_ONE**BIAS_STEPS)
    second_hat = new_second / (1.0 - BETA_TWO**BIAS_STEPS)
    update = first_hat / (jnp.sqrt(second_hat) + EPSILON)
    new_master = master * (1.0 - LEARN_RATE * DECAY) - LEARN_RATE * update
    return (new_master, new_first, new_second)


def pairs(target):
    found = []
    for z in range(NZ):
        for x in range(NX):
            for c in range(NC):
                tz, tx, tc = target(z, x, c)
                found.append(((z * NX + x) * NC + c, ((tz % NZ) * NX + tx % NX) * NC + tc))
    return found


def far(step):
    return lambda z, x, c: (z + (step if z % 2 == 0 else -step), x, c)


def near(step, z_core):
    def target(z, x, c):
        if c != z_core:
            return z, x + (step if x % 2 == 0 else -step), c
        return z + (step if z % 2 == 0 else -step), x, c

    return target


def rows_of(place, piece, partner):
    z, x, c = place // (NX * NC), place // NC % NX, place % NC
    p, q = 1 - 2 * (z % 2), 1 - 2 * (x % 2)
    by_z = (z, z + p, z - p, z - 2 * p)
    by_x = (x, x + q, x - q, x + 2)
    core = 1 - c if partner else c
    rows = []
    for j in range(12):
        k2, k1 = j // 3, j % 3
        row_z = jnp.where(core == 0, by_z[piece], by_z[k2]) + NZ
        row_x = jnp.where(core == 0, by_x[k2], by_x[piece])
        row_z = row_z + (0, -4, 4)[k1] * (1 - 2 * (row_z % 2))
        rows.append(((row_z % NZ) * NX + (row_x + NX) % NX) * NC + core)
    return rows


def put(place, out, pieces):
    count = len(pieces)
    spec = pl.BlockSpec(memory_space=pl.ANY)

    def body(place, *refs):
        refs = refs[0 if out is None else 1 :]
        blocks, whole, sems = refs[:count], refs[count], refs[count + 1]
        copies = []
        for i, (_, piece, partner) in enumerate(pieces):
            for j, row in enumerate(rows_of(place[0], piece, partner)):
                copies.append(pltpu.make_async_copy(blocks[i].at[j], whole.at[row], sems.at[12 * i + j]))
        for copy in copies:
            copy.start()
        for copy in copies:
            copy.wait()

    first = pieces[0][0]
    return pl.pallas_call(
        body,
        out_shape=jax.ShapeDtypeStruct((NZ * NX * NC, *first.shape[1:]), first.dtype),
        in_specs=[pl.BlockSpec(memory_space=pltpu.SMEM)]
        + ([] if out is None else [spec])
        + [pl.BlockSpec(memory_space=pltpu.VMEM)] * count,
        out_specs=spec,
        scratch_shapes=[pltpu.SemaphoreType.DMA((12 * count,))],
        input_output_aliases={} if out is None else {1: 0},
        compiler_params=pltpu.CompilerParams(vmem_limit_bytes=4 * 2**20),
        name="put",
    )(place, *([] if out is None else [out]), *(p[0] for p in pieces))


def gathered(block):
    place = lax.axis_index(FSDP).astype(jnp.int32).reshape(1)
    sent = lambda x, target: lax.ppermute(x, FSDP, pairs(target))
    swap = lambda x: sent(x, lambda z, x, c: (z, x, 1 - c))
    one = jnp.concatenate([block, sent(block, far(4)), sent(block, far(-4))])
    parts = [one]
    for s in (1, -1, 2):
        parts.append(sent(one, near(s, 1)))
    two = jnp.concatenate(parts)
    own = [two]
    for s in (1, -1, 2):
        own.append(sent(two, near(s, 0)))
    other = {0: swap(own[0])}
    out = put(place, None, [(own[0], 0, False), (other[0], 0, True)])
    own[3], out = lax.optimization_barrier((own[3], out))
    other[3] = swap(own[3])
    out = put(place, out, [(own[3], 3, False)])
    own[1], out = lax.optimization_barrier((own[1], out))
    other[1] = swap(own[1])
    out = put(place, out, [(own[1], 1, False), (other[3], 3, True)])
    own[2], out = lax.optimization_barrier((own[2], out))
    other[2] = swap(own[2])
    out = put(place, out, [(own[2], 2, False), (other[1], 1, True)])
    out = put(place, out, [(other[2], 2, True)])
    return out.reshape(1, -1, block.shape[2])


def local(master, first_moment, second_moment, gradient):
    partial_sq = jnp.sum(gradient * gradient)
    squares = taken_together(taken_together(partial_sq, ("section", "fsdp_1", "fsdp_2")), "fsdp_0")
    grad_norm = jnp.sqrt(squares)
    param_count = float(
        lax.axis_size("section")
        * lax.axis_size(FSDP)
        * gradient.shape[0]
        * gradient.shape[1]
        * gradient.shape[2]
    )
    limit = jnp.float32(0.5 * param_count**0.5)
    clip_scale = limit / jnp.maximum(grad_norm, limit)
    grad_rms = grad_norm / jnp.float32(param_count**0.5)
    new_master, new_first, new_second = adamw_part(
        master, first_moment, second_moment, gradient, clip_scale
    )
    weights = gathered(new_master.astype(jnp.bfloat16))
    return (new_master, new_first, new_second, weights, grad_rms)


def solution(mesh):
    torus = Mesh(
        mesh.devices.reshape(mesh.shape["section"], NZ, NX, NC),
        ("section", *FSDP),
    )
    placed = (P("section", FSDP, None),) * 4
    return jax.shard_map(
        local,
        mesh=torus,
        in_specs=placed,
        out_specs=(
            P("section", FSDP, None),
            P("section", FSDP, None),
            P("section", FSDP, None),
            P("section", None, None),
            P(),
        ),
        check_vma=False,
    )
```

```python
import jax
import jax.numpy as jnp
from jax import lax
from jax.experimental import pallas as pl
from jax.experimental.pallas import tpu as pltpu
from jax.sharding import Mesh
from jax.sharding import PartitionSpec as P

FSDP = ("fsdp_0", "fsdp_1", "fsdp_2")
NZ, NX, NC = 12, 4, 2
ROWS_DEV = 8


BETA_ONE = 0.9
BETA_TWO = 0.95
LEARN_RATE = 0.05
DECAY = 0.1
EPSILON = 1e-08
BIAS_STEPS = 10.0


def small(**limits):
    return pltpu.CompilerParams(vmem_limit_bytes=limits.get("mib", 4) * 2**20)


def swapped(x, axis):
    return lax.all_to_all(x, axis, 0, 0, tiled=True)


def spread_squares(count, *state):
    def body(*refs):
        arrays, out, held, sems = refs[:4], refs[4], refs[5:9], refs[9]
        copies = [pltpu.make_async_copy(a, h, sems.at[i]) for i, (a, h) in enumerate(zip(arrays, held))]
        for copy in reversed(copies):
            copy.start()
        copies[-1].wait()
        gradient = held[-1][0]
        lanes = (gradient * gradient).reshape(ROWS_DEV, -1, 128).sum(axis=(0, 1))
        out[...] = jnp.broadcast_to(lanes[None, None], out.shape)
        for copy in copies[:-1]:
            copy.wait()

    return pl.pallas_call(
        body,
        out_shape=[jax.ShapeDtypeStruct((count, 1, 128), jnp.float32)]
        + [jax.ShapeDtypeStruct(a.shape, a.dtype) for a in state],
        in_specs=[pl.BlockSpec(memory_space=pltpu.HBM)] * 4,
        out_specs=[pl.BlockSpec(memory_space=pltpu.VMEM)] * 5,
        scratch_shapes=[pltpu.SemaphoreType.DMA((4,))],
        compiler_params=small(),
        name="spread_squares",
    )(*state)


def summed_and_spread(sums, count):
    def body(s, out):
        out[...] = jnp.broadcast_to(jnp.sum(s[...], axis=0, keepdims=True), out.shape)

    return pl.pallas_call(
        body,
        out_shape=jax.ShapeDtypeStruct((count, 1, 128), jnp.float32),
        in_specs=[pl.BlockSpec(memory_space=pltpu.VMEM)],
        out_specs=pl.BlockSpec(memory_space=pltpu.VMEM),
        compiler_params=small(),
        name="summed_and_spread",
    )(sums)


def norm_of(sums):
    return jnp.sqrt(jnp.sum(sums, axis=(0, 1, 2), keepdims=True)[0])


def adamw_part(master, first_moment, second_moment, gradient, clip_scale):
    scaled = clip_scale * gradient
    new_first = BETA_ONE * first_moment + (1.0 - BETA_ONE) * scaled
    new_second = BETA_TWO * second_moment + (1.0 - BETA_TWO) * scaled * scaled
    first_hat = new_first / (1.0 - BETA_ONE**BIAS_STEPS)
    second_hat = new_second / (1.0 - BETA_TWO**BIAS_STEPS)
    update = first_hat / (jnp.sqrt(second_hat) + EPSILON)
    new_master = master * (1.0 - LEARN_RATE * DECAY) - LEARN_RATE * update
    return (new_master, new_first, new_second)


def stepped(sums, param_count, master, first_moment, second_moment, gradient, weights_only):
    limit = 0.5 * param_count**0.5

    def body(s, p, m, v, g, *outs):
        norm = norm_of(s[...])
        scale = limit / jnp.maximum(norm, limit)
        new = adamw_part(p[0], m[0], v[0], g[0], scale)
        if weights_only:
            outs[0][0] = new[0].astype(jnp.bfloat16)
            return
        for out, value in zip(outs, new):
            out[0] = value
        outs[3][...] = jnp.broadcast_to(norm / param_count**0.5, (1, 128))

    like = lambda dtype: jax.ShapeDtypeStruct(master.shape, dtype)
    out_shape = [like(jnp.bfloat16)] if weights_only else [like(jnp.float32)] * 3 + [jax.ShapeDtypeStruct((1, 128), jnp.float32)]
    return pl.pallas_call(
        body,
        out_shape=out_shape,
        in_specs=[pl.BlockSpec(memory_space=pltpu.VMEM)] * 5,
        out_specs=[pl.BlockSpec(memory_space=pltpu.VMEM)] * len(out_shape),
        compiler_params=small(),
        name="weights" if weights_only else "state",
    )(sums, master, first_moment, second_moment, gradient)


def pairs(target):
    found = []
    for z in range(NZ):
        for x in range(NX):
            for c in range(NC):
                tz, tx, tc = target(z, x, c)
                found.append(((z * NX + x) * NC + c, ((tz % NZ) * NX + tx % NX) * NC + tc))
    return found


def far(step):
    return lambda z, x, c: (z + (step if z % 2 == 0 else -step), x, c)


def near(step, z_core):
    def target(z, x, c):
        if c != z_core:
            return z, x + (step if x % 2 == 0 else -step), c
        return z + (step if z % 2 == 0 else -step), x, c

    return target


def rows_of(place, piece, partner):
    z, x, c = place // (NX * NC), place // NC % NX, place % NC
    p, q = 1 - 2 * (z % 2), 1 - 2 * (x % 2)
    by_z = (z, z + p, z - p, z - 2 * p)
    by_x = (x, x + q, x - q, x + 2)
    core = 1 - c if partner else c
    rows = []
    for j in range(12):
        k2, k1 = j // 3, j % 3
        row_z = jnp.where(core == 0, by_z[piece], by_z[k2]) + NZ
        row_x = jnp.where(core == 0, by_x[k2], by_x[piece])
        row_z = row_z + (0, -4, 4)[k1] * (1 - 2 * (row_z % 2))
        rows.append(((row_z % NZ) * NX + (row_x + NX) % NX) * NC + core)
    return rows


def put(place, out, pieces):
    count = len(pieces)
    spec = pl.BlockSpec(memory_space=pl.ANY)

    def body(place, *refs):
        refs = refs[0 if out is None else 1 :]
        blocks, whole, sems = refs[:count], refs[count], refs[count + 1]
        copies = []
        for i, (_, piece, partner) in enumerate(pieces):
            for j, row in enumerate(rows_of(place[0], piece, partner)):
                copies.append(pltpu.make_async_copy(blocks[i].at[j], whole.at[row], sems.at[12 * i + j]))
        for copy in copies:
            copy.start()
        for copy in copies:
            copy.wait()

    first = pieces[0][0]
    return pl.pallas_call(
        body,
        out_shape=jax.ShapeDtypeStruct((NZ * NX * NC, *first.shape[1:]), first.dtype),
        in_specs=[pl.BlockSpec(memory_space=pltpu.SMEM)]
        + ([] if out is None else [spec])
        + [pl.BlockSpec(memory_space=pltpu.VMEM)] * count,
        out_specs=spec,
        scratch_shapes=[pltpu.SemaphoreType.DMA((12 * count,))],
        input_output_aliases={} if out is None else {1: 0},
        compiler_params=pltpu.CompilerParams(vmem_limit_bytes=4 * 2**20),
        name="put",
    )(place, *([] if out is None else [out]), *(p[0] for p in pieces))


def gathered(block, meanwhile):
    place = lax.axis_index(FSDP).astype(jnp.int32).reshape(1)
    sent = lambda x, target: lax.ppermute(x, FSDP, pairs(target))
    swap = lambda x: sent(x, lambda z, x, c: (z, x, 1 - c))
    above, below, beside = lax.optimization_barrier((sent(block, far(4)), sent(block, far(-4)), meanwhile()))
    one = jnp.concatenate([block, above, below])
    parts = [one]
    for s in (1, -1, 2):
        parts.append(sent(one, near(s, 1)))
    two = jnp.concatenate(parts)
    own = [two]
    for s in (1, -1, 2):
        own.append(sent(two, near(s, 0)))
    other = {0: swap(own[0])}
    out = put(place, None, [(own[0], 0, False), (other[0], 0, True)])
    own[3], out = lax.optimization_barrier((own[3], out))
    other[3] = swap(own[3])
    out = put(place, out, [(own[3], 3, False)])
    own[1], out = lax.optimization_barrier((own[1], out))
    other[1] = swap(own[1])
    other[2] = swap(own[2])
    out = put(place, out, [(own[1], 1, False), (own[2], 2, False), (other[3], 3, True)])
    out = put(place, out, [(other[1], 1, True), (other[2], 2, True)])
    return out.reshape(1, -1, block.shape[2]), beside


def local(master, first_moment, second_moment, gradient):
    param_count = float(
        lax.axis_size("section")
        * lax.axis_size(FSDP)
        * gradient.shape[0]
        * gradient.shape[1]
        * gradient.shape[2]
    )
    plane = ("section", "fsdp_1", "fsdp_2")
    sums, *state = spread_squares(lax.axis_size(plane), master, first_moment, second_moment, gradient)
    sums = swapped(summed_and_spread(swapped(sums, plane), NZ), "fsdp_0")
    (block,) = stepped(sums, param_count, *state, True)
    weights, (new_master, new_first, new_second, rms) = gathered(
        block, lambda: stepped(sums, param_count, *state, False)
    )
    return (new_master, new_first, new_second, weights, rms[0, 0])


def solution(mesh):
    torus = Mesh(
        mesh.devices.reshape(mesh.shape["section"], NZ, NX, NC),
        ("section", *FSDP),
    )
    placed = (P("section", FSDP, None),) * 4
    return jax.shard_map(
        local,
        mesh=torus,
        in_specs=placed,
        out_specs=(
            P("section", FSDP, None),
            P("section", FSDP, None),
            P("section", FSDP, None),
            P("section", None, None),
            P(),
        ),
        check_vma=False,
    )
```

```python
import jax
import jax.numpy as jnp
from jax import lax
from jax.experimental import pallas as pl
from jax.experimental.pallas import tpu as pltpu
from jax.sharding import Mesh
from jax.sharding import PartitionSpec as P

FSDP = ("fsdp_0", "fsdp_1", "fsdp_2")
NZ, NX, NC = 12, 4, 2
ROWS_DEV = 8


BETA_ONE = 0.9
BETA_TWO = 0.95
LEARN_RATE = 0.05
DECAY = 0.1
EPSILON = 1e-08
BIAS_STEPS = 10.0


def small(**limits):
    return pltpu.CompilerParams(vmem_limit_bytes=limits.get("mib", 4) * 2**20)


def swapped(x, axis):
    return lax.all_to_all(x, axis, 0, 0, tiled=True)


def spread_squares(count, *state):
    def body(*refs):
        arrays, out, held, sems = refs[:4], refs[4], refs[5:9], refs[9]
        copies = [pltpu.make_async_copy(a, h, sems.at[i]) for i, (a, h) in enumerate(zip(arrays, held))]
        for copy in reversed(copies):
            copy.start()
        copies[-1].wait()
        gradient = held[-1][0]
        lanes = (gradient * gradient).reshape(ROWS_DEV, -1, 128).sum(axis=(0, 1))
        out[...] = jnp.broadcast_to(lanes[None, None], out.shape)
        for copy in copies[:-1]:
            copy.wait()

    return pl.pallas_call(
        body,
        out_shape=[jax.ShapeDtypeStruct((count, 1, 128), jnp.float32)]
        + [jax.ShapeDtypeStruct(a.shape, a.dtype) for a in state],
        in_specs=[pl.BlockSpec(memory_space=pltpu.HBM)] * 4,
        out_specs=[pl.BlockSpec(memory_space=pltpu.VMEM)] * 5,
        scratch_shapes=[pltpu.SemaphoreType.DMA((4,))],
        compiler_params=pltpu.CompilerParams(vmem_limit_bytes=54656 * 1024),
        name="spread_squares",
    )(*state)


def summed_and_spread(sums, count):
    def body(s, out):
        out[...] = jnp.broadcast_to(jnp.sum(s[...], axis=0, keepdims=True), out.shape)

    return pl.pallas_call(
        body,
        out_shape=jax.ShapeDtypeStruct((count, 1, 128), jnp.float32),
        in_specs=[pl.BlockSpec(memory_space=pltpu.VMEM)],
        out_specs=pl.BlockSpec(memory_space=pltpu.VMEM),
        compiler_params=small(),
        name="summed_and_spread",
    )(sums)


def norm_of(sums):
    return jnp.sqrt(jnp.sum(sums, axis=(0, 1, 2), keepdims=True)[0])


def adamw_part(master, first_moment, second_moment, gradient, clip_scale):
    scaled = clip_scale * gradient
    new_first = BETA_ONE * first_moment + (1.0 - BETA_ONE) * scaled
    new_second = BETA_TWO * second_moment + (1.0 - BETA_TWO) * scaled * scaled
    first_hat = new_first / (1.0 - BETA_ONE**BIAS_STEPS)
    second_hat = new_second / (1.0 - BETA_TWO**BIAS_STEPS)
    update = first_hat / (jnp.sqrt(second_hat) + EPSILON)
    new_master = master * (1.0 - LEARN_RATE * DECAY) - LEARN_RATE * update
    return (new_master, new_first, new_second)


def stepped(sums, param_count, master, first_moment, second_moment, gradient, weights_only):
    limit = 0.5 * param_count**0.5

    def body(s, p, m, v, g, *outs):
        norm = norm_of(s[...])
        scale = limit / jnp.maximum(norm, limit)
        new = adamw_part(p[0], m[0], v[0], g[0], scale)
        if weights_only:
            outs[0][0] = new[0].astype(jnp.bfloat16)
            return
        for out, value in zip(outs, new):
            out[0] = value
        outs[3][...] = jnp.broadcast_to(norm / param_count**0.5, (1, 128))

    like = lambda dtype: jax.ShapeDtypeStruct(master.shape, dtype)
    out_shape = [like(jnp.bfloat16)] if weights_only else [like(jnp.float32)] * 3 + [jax.ShapeDtypeStruct((1, 128), jnp.float32)]
    return pl.pallas_call(
        body,
        out_shape=out_shape,
        in_specs=[pl.BlockSpec(memory_space=pltpu.VMEM)] * 5,
        out_specs=[pl.BlockSpec(memory_space=pltpu.VMEM)] * len(out_shape),
        compiler_params=small(),
        name="weights" if weights_only else "state",
    )(sums, master, first_moment, second_moment, gradient)


def pairs(target):
    found = []
    for z in range(NZ):
        for x in range(NX):
            for c in range(NC):
                tz, tx, tc = target(z, x, c)
                found.append(((z * NX + x) * NC + c, ((tz % NZ) * NX + tx % NX) * NC + tc))
    return found


def far(step):
    return lambda z, x, c: (z + (step if z % 2 == 0 else -step), x, c)


def near(step, z_core):
    def target(z, x, c):
        if c != z_core:
            return z, x + (step if x % 2 == 0 else -step), c
        return z + (step if z % 2 == 0 else -step), x, c

    return target


def rows_of(place, piece, partner):
    z, x, c = place // (NX * NC), place // NC % NX, place % NC
    p, q = 1 - 2 * (z % 2), 1 - 2 * (x % 2)
    by_z = (z, z + p, z - p, z - 2 * p)
    by_x = (x, x + q, x - q, x + 2)
    core = 1 - c if partner else c
    rows = []
    for j in range(12):
        k2, k1 = j // 3, j % 3
        row_z = jnp.where(core == 0, by_z[piece], by_z[k2]) + NZ
        row_x = jnp.where(core == 0, by_x[k2], by_x[piece])
        row_z = row_z + (0, -4, 4)[k1] * (1 - 2 * (row_z % 2))
        rows.append(((row_z % NZ) * NX + (row_x + NX) % NX) * NC + core)
    return rows


def put(place, out, pieces):
    count = len(pieces)
    spec = pl.BlockSpec(memory_space=pl.ANY)

    def body(place, *refs):
        refs = refs[0 if out is None else 1 :]
        blocks, whole, sems = refs[:count], refs[count], refs[count + 1]
        copies = []
        for i, (_, piece, partner) in enumerate(pieces):
            for j, row in enumerate(rows_of(place[0], piece, partner)):
                copies.append(pltpu.make_async_copy(blocks[i].at[j], whole.at[row], sems.at[12 * i + j]))
        for copy in copies:
            copy.start()
        for copy in copies:
            copy.wait()

    first = pieces[0][0]
    return pl.pallas_call(
        body,
        out_shape=jax.ShapeDtypeStruct((NZ * NX * NC, *first.shape[1:]), first.dtype),
        in_specs=[pl.BlockSpec(memory_space=pltpu.SMEM)]
        + ([] if out is None else [spec])
        + [pl.BlockSpec(memory_space=pltpu.VMEM)] * count,
        out_specs=spec,
        scratch_shapes=[pltpu.SemaphoreType.DMA((12 * count,))],
        input_output_aliases={} if out is None else {1: 0},
        compiler_params=pltpu.CompilerParams(vmem_limit_bytes=4 * 2**20),
        name="put",
    )(place, *([] if out is None else [out]), *(p[0] for p in pieces))


def gathered(block, meanwhile):
    place = lax.axis_index(FSDP).astype(jnp.int32).reshape(1)
    sent = lambda x, target: lax.ppermute(x, FSDP, pairs(target))
    swap = lambda x: sent(x, lambda z, x, c: (z, x, 1 - c))
    above, below, beside = lax.optimization_barrier((sent(block, far(4)), sent(block, far(-4)), meanwhile()))
    one = jnp.concatenate([block, above, below])
    parts = [one]
    for s in (1, -1, 2):
        parts.append(sent(one, near(s, 1)))
    two = jnp.concatenate(parts)
    own = [two]
    for s in (1, -1, 2):
        own.append(sent(two, near(s, 0)))
    other = {0: swap(own[0])}
    out = put(place, None, [(own[0], 0, False)])
    own[3], out = lax.optimization_barrier((own[3], out))
    other[3] = swap(own[3])
    out = put(place, out, [(own[3], 3, False), (other[0], 0, True)])
    own[1], out = lax.optimization_barrier((own[1], out))
    other[1] = swap(own[1])
    other[2] = swap(own[2])
    out = put(place, out, [(own[1], 1, False), (own[2], 2, False), (other[3], 3, True)])
    out = put(place, out, [(other[1], 1, True), (other[2], 2, True)])
    return out.reshape(1, -1, block.shape[2]), beside


def local(master, first_moment, second_moment, gradient):
    param_count = float(
        lax.axis_size("section")
        * lax.axis_size(FSDP)
        * gradient.shape[0]
        * gradient.shape[1]
        * gradient.shape[2]
    )
    plane = ("section", "fsdp_1", "fsdp_2")
    sums, *state = spread_squares(lax.axis_size(plane), master, first_moment, second_moment, gradient)
    sums = swapped(summed_and_spread(swapped(sums, plane), NZ), "fsdp_0")
    (block,) = stepped(sums, param_count, *state, True)
    weights, (new_master, new_first, new_second, rms) = gathered(
        block, lambda: stepped(sums, param_count, *state, False)
    )
    return (new_master, new_first, new_second, weights, rms[0, 0])


def solution(mesh):
    torus = Mesh(
        mesh.devices.reshape(mesh.shape["section"], NZ, NX, NC),
        ("section", *FSDP),
    )
    placed = (P("section", FSDP, None),) * 4
    return jax.shard_map(
        local,
        mesh=torus,
        in_specs=placed,
        out_specs=(
            P("section", FSDP, None),
            P("section", FSDP, None),
            P("section", FSDP, None),
            P("section", None, None),
            P(),
        ),
        check_vma=False,
    )
```
